256 devices in a mesh: dp: 2 (over core), seq: 32 (over z, x), tensor: 4 (over y).
Axes of the slice: x: 4, y: 4, z: 8, core: 2. Of those that a mesh axis runs over, the one named last changes fastest.
Arguments:
- tokens: bfloat16 [2048, 4, 5120], P('seq', 'dp'), parts along dimension 1, may hold values from -6 to 6
- w_query: bfloat16 [5120, 5120], P(None, 'tensor'), may hold values from -0.5 to 0.5, as said below
- w_key: bfloat16 [5120, 5120], P(None, 'tensor'), may hold values from -0.5 to 0.5, as said below
- w_value: bfloat16 [5120, 5120], P(None, 'tensor'), may hold values from -0.078125 to 0.078125
- w_out: bfloat16 [5120, 5120], P('tensor'), may hold values from -0.125 to 0.125
- gain_query: float32 [5120], P('tensor'), may hold values from 0.5 to 4
- gain_key: float32 [5120], P('tensor'), may hold values from 0.5 to 4
Outputs:
- attended: bfloat16 [2048, 4, 5120], P(('seq', 'tensor'), 'dp'), parts along dimension 1
The draws below stay inside these ranges and needn't reach their ends.
There are 2 independent parts, one for each index of `dp`. The reference program is written for one: setup_inputs(seed, part) draws one part's arguments, and reference() takes and returns one part's arrays. A program takes and returns all parts, laid end to end along the dimension named above; an argument that names none is the same for every part. Nothing has to cross between parts.
Inputs may be any that keep to these rules, and one draw needn't show every extreme that they name: `w_query`: entries of order 5120 ** -0.5 with unequal column scales. `w_key`: entries of order 5120 ** -0.5 with unequal column scales.
All inputs are finite; a program needn't handle non-finite values.
Results may differ from the reference program's by a relative error of at most 0.013.
The reference program's roundings to bfloat16 on the way count: a program that leaves them out, or rounds other values in their place, can miss the bound.
Values may be sent and summed in bfloat16 or wider, within the bound.
A program may use at most 256 MiB of HBM per device.

```python
import jax
import jax.numpy as jnp
from jax import lax

D = 5120
HEADS = 40
HEAD_DIM = 128
SEQS = 2
TOK_DEV = 64
SEQ = 2048


def ramped_weight(key, salt):
    width = HEADS * HEAD_DIM
    first, second = jax.random.split(jax.random.fold_in(key, salt))
    base = jax.random.truncated_normal(first, -4.0, 4.0, (D, width), jnp.float32)
    heads = (jnp.arange(width) // HEAD_DIM).astype(jnp.float32)
    ramp = jnp.exp(jnp.log(0.6) + jnp.log(3.0) * heads / max(HEADS - 1, 1))
    upper = 3.3
    column = jnp.exp(jax.random.uniform(second, (width,), jnp.float32) * jnp.log(upper))
    scaled = base * (ramp * column)[None, :] / jnp.sqrt(jnp.float32(D))
    return jnp.clip(scaled, -0.5, 0.5).astype(jnp.bfloat16)


def drawn_gain(key, salt):
    width = HEADS * HEAD_DIM
    lower, upper = (0.5, 2.0)
    sample = jax.random.uniform(jax.random.fold_in(key, salt), (width,), jnp.float32, jnp.log(lower), jnp.log(upper))
    return jnp.exp(sample).astype(jnp.float32)


def draw_w_query(key, part):
    return ramped_weight(key, 11)


def draw_w_key(key, part):
    return ramped_weight(key, 23)


def draw_gain_query(key, part):
    return drawn_gain(key, 37)


def draw_gain_key(key, part):
    return drawn_gain(key, 41)


def with_spikes(entries, rng, source, target, parts, factor):
    def block_of(axis_at):
        return (jnp.arange(entries.shape[axis_at]) // (entries.shape[axis_at] // parts)).reshape((-1,) + (1,) * (entries.ndim - 1 - axis_at))

    one_side = jax.random.permutation(rng, parts)[block_of(target)]
    other_side = (block_of(target) + parts // 2) % parts
    return jnp.where((block_of(source) == one_side) | (block_of(source) == other_side), factor * entries, entries)


def steps_of(key, dims, shards, smallest, largest):
    level = 1.0
    for axis_at, parts in shards:
        heights = jax.random.uniform(jax.random.fold_in(jax.random.fold_in(key, 6), axis_at), (parts,), jnp.float32, smallest / len(shards), largest / len(shards))
        level = level * jnp.repeat(jnp.exp(heights), dims[axis_at] // parts).reshape((-1,) + (1,) * (len(dims) - 1 - axis_at))
    return level


def bell_draw(key, dims, spread, reach, cuts=(), held_as=jnp.bfloat16):
    loudness = steps_of(key, dims, cuts, -0.22, 0.18) if cuts else 1.0
    entries = jax.random.normal(key, dims, jnp.float32) * spread * loudness
    return jnp.minimum(jnp.maximum(entries, -reach), reach).astype(held_as)


def bell_draw_with(key, dims, scale, reach, cuts, heavy, kind=jnp.bfloat16):
    drawn = scale * jax.random.normal(key, dims, jnp.float32)
    if cuts:
        drawn = drawn * steps_of(key, dims, cuts, -0.22, 0.18)
    return jnp.clip(with_spikes(drawn, jax.random.fold_in(key, 3), *heavy), -reach, reach).astype(kind)


def setup_inputs(seed: int = 0, part: int = 0) -> dict:
    seeds = jax.random.split(jax.random.key(seed), 8)
    part_splits = jax.random.split(jax.random.fold_in(seeds[7], part), 8)
    return {
        "tokens": bell_draw(part_splits[0], (SEQ, SEQS, D), 1.0, 6.0, ((0, 32),)),
        "w_query": draw_w_query(jax.random.fold_in(seeds[7], 71), part),
        "w_key": draw_w_key(jax.random.fold_in(seeds[7], 71), part),
        "w_value": bell_draw(seeds[3], (D, HEADS * HEAD_DIM), D ** -0.5, 0.078125, ((1, 4),)),
        "w_out": bell_draw_with(seeds[4], (HEADS * HEAD_DIM, D), (HEADS * HEAD_DIM) ** -0.5, 0.125, ((0, 4),), (0, 1, 4, 2.0)),
        "gain_query": draw_gain_query(jax.random.fold_in(seeds[7], 71), part),
        "gain_key": draw_gain_key(jax.random.fold_in(seeds[7], 71), part),
    }


def rotary(field, positions):
    half = HEAD_DIM // 2
    shaped = field.reshape(field.shape[0], -1, HEAD_DIM)
    freqs = jnp.exp(-jnp.log(500000.0) * jnp.arange(half, dtype=jnp.float32) * 2.0 / HEAD_DIM)
    angle = positions.astype(jnp.float32)[:, None] * freqs[None, :]
    cosine = jnp.cos(angle)[:, None, :]
    sine = jnp.sin(angle)[:, None, :]
    first = shaped[..., :half]
    second = shaped[..., half:]
    turned = jnp.concatenate([first * cosine - second * sine, second * cosine + first * sine], axis=-1)
    return turned.reshape(field.shape[0], -1)

def one_sequence(seq_tokens, w_query, w_key, w_value, w_out, gain_query, gain_key):
    width = HEADS * HEAD_DIM
    query = jnp.dot(seq_tokens, w_query, preferred_element_type=jnp.float32)
    key_raw = jnp.dot(seq_tokens, w_key, preferred_element_type=jnp.float32)
    value = jnp.dot(seq_tokens, w_value, preferred_element_type=jnp.float32).astype(jnp.bfloat16)
    scale_q = lax.rsqrt(lax.optimization_barrier(jnp.sum(query * query, axis=1)) / width + 1e-06)
    scale_k = lax.rsqrt(lax.optimization_barrier(jnp.sum(key_raw * key_raw, axis=1)) / width + 1e-06)
    positions = jnp.arange(SEQ, dtype=jnp.int32)
    q_normed = rotary(query * scale_q[:, None] * gain_query[None, :], positions).astype(jnp.bfloat16)
    k_normed = rotary(key_raw * scale_k[:, None] * gain_key[None, :], positions).astype(jnp.bfloat16)
    keys_all = k_normed.reshape(SEQ, HEADS, HEAD_DIM).astype(jnp.float32)
    values_all = value.reshape(SEQ, HEADS, HEAD_DIM).astype(jnp.float32)
    factor = HEAD_DIM ** (-0.5)

    def one_block(index):
        start = (index * TOK_DEV).astype(jnp.int32)
        q_block = lax.dynamic_slice_in_dim(q_normed, start, TOK_DEV, 0).reshape(TOK_DEV, HEADS, HEAD_DIM).astype(jnp.float32)
        scores = jnp.einsum('qhd,khd->hqk', q_block, keys_all) * factor
        q_pos = start + jnp.arange(TOK_DEV, dtype=jnp.int32)
        allowed = positions[None, None, :] <= q_pos[None, :, None]
        top = lax.optimization_barrier(jnp.max(jnp.where(allowed, scores, -1e+30), axis=2))
        expo = jnp.where(allowed, jnp.exp(scores - top[..., None]), 0.0)
        total = lax.optimization_barrier(jnp.sum(expo, axis=2))
        rounded = expo.astype(jnp.bfloat16).astype(jnp.float32)
        summed = jnp.einsum('hqk,khd->hqd', rounded, values_all)
        mixed = (summed / total[..., None]).astype(jnp.bfloat16)
        return jnp.transpose(mixed, (1, 0, 2)).reshape(TOK_DEV, width)
    blocks = lax.map(one_block, jnp.arange(SEQ // TOK_DEV, dtype=jnp.int32))
    mixed_all = blocks.reshape(SEQ, width)
    return jnp.dot(mixed_all, w_out, preferred_element_type=jnp.float32).astype(jnp.bfloat16)

def reference(tokens, w_query, w_key, w_value, w_out, gain_query, gain_key):
    by_sequence = jnp.transpose(tokens, (1, 0, 2))

    def handle(seq_tokens):
        return one_sequence(seq_tokens, w_query, w_key, w_value, w_out, gain_query, gain_key)
    results = lax.map(handle, by_sequence)
    return jnp.transpose(results, (1, 0, 2))
```

```python
import functools

import jax
import jax.numpy as jnp
import numpy as np
from jax import lax
from jax.experimental import pallas as pl
from jax.experimental.pallas import tpu as pltpu
from jax.sharding import PartitionSpec as P

HEADS = 40
HEAD_DIM = 128
D = 5120
SEQ_DEV = 32
TENSOR = 4
ROWS = 64
PAIR_ROWS = 128
LOCAL = 1280
TILES = 5
WIDE = 256
SLOTS = 4
AHEAD = 3
CHUNK = 512
QB = 256
MESH = pl.DeviceIdType.MESH
F32 = jnp.float32
BF16 = jnp.bfloat16


def pair_device(tile, x):
    z = lax.rem((8 * tile) // 5 + 2 * x, 8)
    return z * 4 + x


def kernel(x_ref, gq_ref, gk_ref, freq_ref, wq_hbm, wk_hbm, wv_hbm, wo_hbm, out_ref,
           wbuf, wobuf, raw, send, recv, amix, mixed, perm, part, osend, orecv, oself,
           ssend, srecv, tabs, wsem, wosem, send_sem, recv_sem, mix_send_sem, mix_sem,
           ss_send_sem, ss_sem, o_send_sem, o_sem):
    me = lax.axis_index("seq")
    t = lax.axis_index("tensor")
    barrier = pltpu.get_barrier_semaphore()

    def greet(d, _):
        pl.semaphore_signal(barrier, inc=1, device_id={"seq": lax.rem(me + d, SEQ_DEV)}, device_id_type=MESH)
        return 0

    lax.fori_loop(1, SEQ_DEV, greet, 0)
    for d in range(1, TENSOR):
        pl.semaphore_signal(barrier, inc=1, device_id={"tensor": lax.rem(t + d, TENSOR)}, device_id_type=MESH)

    weights = (wv_hbm, wk_hbm, wq_hbm)

    def tile_at(s):
        return lax.rem(s + me, TILES)

    def w_copy(mat, s):
        slot = lax.rem(mat * TILES + s, SLOTS)
        cols = pl.ds(pl.multiple_of(tile_at(s) * WIDE, WIDE), WIDE)
        return pltpu.make_async_copy(weights[mat].at[:, cols], wbuf.at[slot], wsem.at[slot])

    for s in range(AHEAD):
        w_copy(0, s).start()

    def prefetch(mat, s):
        later = s + AHEAD

        @pl.when(later < TILES)
        def _():
            w_copy(mat, later).start()

        if mat < 2:
            @pl.when(later >= TILES)
            def _():
                w_copy(mat + 1, later - TILES).start()

    def product(mat, s):
        prefetch(mat, s)
        w_copy(mat, s).wait()
        slot = lax.rem(mat * TILES + s, SLOTS)
        return jnp.dot(x_ref[...], wbuf[slot], preferred_element_type=F32)

    def send_tile(mat, tile, blocks):
        for x in range(4):
            send[mat, tile * 4 + x] = blocks[x]
        for x in range(4):
            dest = pair_device(tile, x)
            src = send.at[mat, tile * 4 + x]
            dst = recv.at[mat, pl.ds(pl.multiple_of(me * ROWS, ROWS), ROWS), :]

            @pl.when(dest != me)
            def _():
                pltpu.make_async_remote_copy(
                    src_ref=src, dst_ref=dst, send_sem=send_sem.at[mat], recv_sem=recv_sem.at[mat],
                    device_id={"seq": dest}, device_id_type=MESH).start()

            @pl.when(dest == me)
            def _():
                pltpu.make_async_copy(src, dst, recv_sem.at[mat]).start()

    lane = lax.broadcasted_iota(jnp.int32, (ROWS, HEAD_DIM), 1)
    pos = lax.broadcasted_iota(jnp.int32, (ROWS, HEAD_DIM), 0) + me * ROWS
    angle = pos.astype(F32) * freq_ref[...]
    sine = jnp.sin(angle)
    tabs[0] = jnp.cos(angle)
    tabs[1] = jnp.where(lane < HEAD_DIM // 2, -sine, sine)

    pl.semaphore_wait(barrier, SEQ_DEV - 1 + TENSOR - 1)

    def v_step(s, _):
        y = product(0, s).astype(BF16)
        send_tile(0, tile_at(s), [y[j * ROWS:(j + 1) * ROWS, hh * 128:(hh + 1) * 128]
                                  for hh in range(2) for j in range(2)])
        return 0

    lax.fori_loop(0, TILES, v_step, 0)

    def kq_step(mat, s, acc):
        y = product(mat, s)
        raw[mat - 1, :, pl.ds(pl.multiple_of(tile_at(s) * WIDE, WIDE), WIDE)] = y
        return acc + (y[:, :128] * y[:, :128] + y[:, 128:] * y[:, 128:])

    rows_i = lax.broadcasted_iota(jnp.int32, (PAIR_ROWS, PAIR_ROWS), 0)
    cols_i = lax.broadcasted_iota(jnp.int32, (PAIR_ROWS, PAIR_ROWS), 1)
    eye = rows_i == cols_i

    def ss_copy(mat, d):
        return pltpu.make_async_remote_copy(
            src_ref=ssend.at[mat - 1], dst_ref=srecv.at[mat - 1, d - 1],
            send_sem=ss_send_sem.at[mat - 1, d - 1], recv_sem=ss_sem.at[mat - 1, d - 1],
            device_id={"tensor": lax.rem(t + d, TENSOR)}, device_id_type=MESH)

    def send_sums(mat, acc):
        col = jnp.sum(acc, axis=1, keepdims=True)
        row = jnp.sum(jnp.where(eye, col, 0.0), axis=0, keepdims=True)
        ssend[mat - 1] = jnp.broadcast_to(row, (8, PAIR_ROWS))
        for d in range(1, TENSOR):
            ss_copy(mat, d).start()

    def norm_send(mat, gain_ref):
        total = ssend[mat - 1]
        for d in range(1, TENSOR):
            ss_copy(mat, d).wait_recv()
            total = total + srecv[mat - 1, d - 1]
        col = jnp.sum(jnp.where(eye, total[0:1, :], 0.0), axis=1, keepdims=True)
        scale = lax.rsqrt(col / float(HEADS * HEAD_DIM) + 1e-06)

        def step(s, _):
            tile = tile_at(s)
            cols = pl.ds(pl.multiple_of(tile * WIDE, WIDE), WIDE)
            y = raw[mat - 1, :, cols] * scale * gain_ref[:, cols]
            blocks = []
            for hh in range(2):
                for j in range(2):
                    u = y[j * ROWS:(j + 1) * ROWS, hh * 128:(hh + 1) * 128]
                    turned = u * tabs[0] + pltpu.roll(u, HEAD_DIM // 2, 1) * tabs[1]
                    blocks.append(turned.astype(BF16))
            send_tile(mat, tile, blocks)
            return 0

        lax.fori_loop(0, TILES, step, 0)

    zero = jnp.zeros((PAIR_ROWS, 128), F32)
    acc = lax.fori_loop(0, TILES, lambda s, a: kq_step(1, s, a), zero)
    send_sums(1, acc)
    acc = lax.fori_loop(0, 3, lambda s, a: kq_step(2, s, a), zero)
    norm_send(1, gk_ref)
    acc = lax.fori_loop(3, TILES, lambda s, a: kq_step(2, s, a), acc)
    send_sums(2, acc)
    wo_copy = pltpu.make_async_copy(wo_hbm, wobuf, wosem)
    wo_copy.start()
    norm_send(2, gq_ref)

    my_z = me // 4
    my_x = lax.rem(me, 4)
    shifted = lax.rem(my_z + 8 - 2 * my_x + 8, 8)
    my_tile = (5 * shifted + 4) // 8
    attends = (8 * my_tile) // 5 == shifted
    head = my_tile * 2 + my_x // 2
    j_mine = lax.rem(my_x, 2)

    @pl.when(attends)
    def _():
        for mat in range(3):
            pltpu.make_async_copy(recv.at[mat], recv.at[mat], recv_sem.at[mat]).wait()
        scale = float(HEAD_DIM ** -0.5 * np.log2(np.e))
        diag = (lax.broadcasted_iota(jnp.int32, (QB, QB), 0) >= lax.broadcasted_iota(jnp.int32, (QB, QB), 1))
        for b in range(SEQ_DEV * ROWS // QB):
            q = recv[2, b * QB:(b + 1) * QB, :]
            last = lax.dot_general(q, recv[1, b * QB:(b + 1) * QB, :], (((1,), (1,)), ((), ())),
                                   preferred_element_type=F32)
            last = jnp.where(diag, last, -1e30)
            top = jnp.max(last, axis=1, keepdims=True)
            if b > 0:
                past = lax.dot_general(q, recv[1, 0:b * QB, :], (((1,), (1,)), ((), ())),
                                       preferred_element_type=F32)
                top = jnp.maximum(top, jnp.max(past, axis=1, keepdims=True))
                e_past = jnp.exp2((past - top) * scale)
            e_last = jnp.exp2((last - top) * scale)
            total = jnp.sum(e_last, axis=1, keepdims=True)
            o = jnp.dot(e_last.astype(BF16), recv[0, b * QB:(b + 1) * QB, :], preferred_element_type=F32)
            if b > 0:
                total = total + jnp.sum(e_past, axis=1, keepdims=True)
                o = o + jnp.dot(e_past.astype(BF16), recv[0, 0:b * QB, :], preferred_element_type=F32)
            amix[b * QB:(b + 1) * QB, :] = (o / total).astype(BF16)
            for k in range(QB // ROWS):
                dest = b * (QB // ROWS) + k
                src = amix.at[pl.ds(dest * ROWS, ROWS), :]
                dst = mixed.at[pl.ds(pl.multiple_of(j_mine * ROWS, ROWS), ROWS),
                               pl.ds(pl.multiple_of(head * 128, 128), 128)]

                @pl.when(dest != me)
                def _():
                    pltpu.make_async_remote_copy(
                        src_ref=src, dst_ref=dst, send_sem=mix_send_sem, recv_sem=mix_sem,
                        device_id={"seq": jnp.int32(dest)}, device_id_type=MESH).start()

                @pl.when(dest == me)
                def _():
                    pltpu.make_async_copy(src, dst, mix_sem).start()

    wo_copy.wait()
    pltpu.make_async_copy(mixed, mixed, mix_sem).wait()
    swap = (cols_i == lax.rem(rows_i, 2) * ROWS + rows_i // 2).astype(F32).astype(BF16)
    perm[...] = jnp.dot(swap, mixed[...], preferred_element_type=F32).astype(BF16)
    out_rows = PAIR_ROWS // TENSOR

    def o_step(c, _):
        cols = pl.ds(pl.multiple_of(c * CHUNK, CHUNK), CHUNK)
        y = jnp.dot(perm[...], wobuf[:, cols], preferred_element_type=F32)
        part[...] = y
        osend[:, cols] = y.astype(BF16)
        oself[:, cols] = part[pl.ds(pl.multiple_of(t * out_rows, out_rows), out_rows), :]
        for d in range(1, TENSOR):
            peer = lax.rem(t + d, TENSOR)
            pltpu.make_async_remote_copy(
                src_ref=osend.at[pl.ds(pl.multiple_of(peer * out_rows, out_rows), out_rows), cols],
                dst_ref=orecv.at[d - 1, :, cols],
                send_sem=o_send_sem.at[d - 1], recv_sem=o_sem.at[d - 1],
                device_id={"tensor": peer}, device_id_type=MESH).start()
        return 0

    lax.fori_loop(0, D // CHUNK, o_step, 0)
    for d in range(1, TENSOR):
        pltpu.make_async_copy(orecv.at[d - 1], orecv.at[d - 1], o_sem.at[d - 1]).wait()

    def sum_step(c, _):
        cols = pl.ds(pl.multiple_of(c * CHUNK, CHUNK), CHUNK)
        y = oself[:, cols]
        for d in range(1, TENSOR):
            y = y + orecv[d - 1, :, cols].astype(F32)
        out_ref[:, cols] = y.astype(BF16)
        return 0

    lax.fori_loop(0, D // CHUNK, sum_step, 0)

    for mat in range(1, 3):
        for d in range(1, TENSOR):
            ss_copy(mat, d).wait_send()
    for d in range(1, TENSOR):
        pltpu.make_async_copy(orecv.at[d - 1], orecv.at[d - 1], o_send_sem.at[d - 1]).wait()

    @pl.when(attends)
    def _():
        for mat in range(3):
            left = send.at[mat, pl.ds(0, 4 * TILES - 1)]
            pltpu.make_async_copy(left, left, send_sem.at[mat]).wait()
        left = amix.at[pl.ds(0, (SEQ_DEV - 1) * ROWS), :]
        pltpu.make_async_copy(left, left, mix_send_sem).wait()

    @pl.when(jnp.logical_not(attends))
    def _():
        for mat in range(3):
            pltpu.make_async_copy(send.at[mat], send.at[mat], send_sem.at[mat]).wait()


def local(tokens, w_query, w_key, w_value, w_out, gain_query, gain_key):
    flat = jnp.transpose(tokens, (1, 0, 2)).reshape(PAIR_ROWS, D)
    half = HEAD_DIM // 2
    freqs = jnp.exp(-jnp.log(500000.0) * jnp.arange(half, dtype=F32) * 2.0 / HEAD_DIM)
    freq_row = jnp.concatenate([freqs, freqs])[None, :]
    dma = pltpu.SemaphoreType.DMA
    vmem = pl.BlockSpec(memory_space=pltpu.VMEM)
    hbm = pl.BlockSpec(memory_space=pl.ANY)
    out_rows = PAIR_ROWS // TENSOR
    out = pl.pallas_call(
        kernel,
        out_shape=jax.ShapeDtypeStruct((out_rows, D), BF16),
        in_specs=[vmem] * 4 + [hbm] * 4,
        out_specs=vmem,
        scratch_shapes=[
            pltpu.VMEM((SLOTS, D, WIDE), BF16),
            pltpu.VMEM((LOCAL, D), BF16),
            pltpu.VMEM((2, PAIR_ROWS, LOCAL), F32),
            pltpu.VMEM((3, 4 * TILES, ROWS, 128), BF16),
            pltpu.VMEM((3, SEQ_DEV * ROWS, 128), BF16),
            pltpu.VMEM((SEQ_DEV * ROWS, 128), BF16),
            pltpu.VMEM((PAIR_ROWS, LOCAL), BF16),
            pltpu.VMEM((PAIR_ROWS, LOCAL), BF16),
            pltpu.VMEM((PAIR_ROWS, CHUNK), F32),
            pltpu.VMEM((PAIR_ROWS, D), BF16),
            pltpu.VMEM((TENSOR - 1, out_rows, D), BF16),
            pltpu.VMEM((out_rows, D), F32),
            pltpu.VMEM((2, 8, PAIR_ROWS), F32),
            pltpu.VMEM((2, TENSOR - 1, 8, PAIR_ROWS), F32),
            pltpu.VMEM((2, ROWS, HEAD_DIM), F32),
            dma((SLOTS,)), dma, dma((3,)), dma((3,)), dma, dma,
            dma((2, TENSOR - 1)), dma((2, TENSOR - 1)), dma((TENSOR - 1,)), dma((TENSOR - 1,)),
        ],
        compiler_params=pltpu.CompilerParams(
            collective_id=0, has_side_effects=True, vmem_limit_bytes=60 * 1024 * 1024),
        name="layer",
    )(flat, gain_query[None, :], gain_key[None, :], freq_row, w_query, w_key, w_value, w_out)
    return out.reshape(out_rows // 2, 2, D)


def solution(mesh):
    return jax.shard_map(
        local,
        mesh=mesh,
        in_specs=(
            P("seq", "dp", None),
            P(None, "tensor"),
            P(None, "tensor"),
            P(None, "tensor"),
            P("tensor", None),
            P("tensor"),
            P("tensor"),
        ),
        out_specs=P(("seq", "tensor"), "dp", None),
        check_vma=False,
    )
```

```python
import functools

import jax
import jax.numpy as jnp
import numpy as np
from jax import lax
from jax.experimental import pallas as pl
from jax.experimental.pallas import tpu as pltpu
from jax.sharding import PartitionSpec as P

HEADS = 40
HEAD_DIM = 128
D = 5120
SEQ_DEV = 32
TENSOR = 4
ROWS = 64
PAIR_ROWS = 128
LOCAL = 1280
TILES = 5
WIDE = 256
SLOTS = 4
AHEAD = 3
CHUNK = 512
QB = 256
MESH = pl.DeviceIdType.MESH
F32 = jnp.float32
BF16 = jnp.bfloat16


def pair_device(tile, x):
    z = lax.rem((8 * tile) // 5 + 2 * x, 8)
    return z * 4 + x


def kernel(tok_hbm, gq_ref, gk_ref, freq_ref, wq_hbm, wk_hbm, wv_hbm, wo_hbm, out_ref,
           tok, x_ref, wbuf, wobuf, raw, send, recv, amix, mixed, perm, part, osend, orecv, oself,
           ssend, srecv, tabs, tok_sem, wsem, wosem, send_sem, recv_sem, mix_send_sem, mix_sem,
           ss_send_sem, ss_sem, o_send_sem, o_sem):
    me = lax.axis_index("seq")
    t = lax.axis_index("tensor")
    barrier = pltpu.get_barrier_semaphore()

    def greet(d, _):
        pl.semaphore_signal(barrier, inc=1, device_id={"seq": lax.rem(me + d, SEQ_DEV)}, device_id_type=MESH)
        return 0

    lax.fori_loop(1, SEQ_DEV, greet, 0)
    for d in range(1, TENSOR):
        pl.semaphore_signal(barrier, inc=1, device_id={"tensor": lax.rem(t + d, TENSOR)}, device_id_type=MESH)

    weights = (wv_hbm, wk_hbm, wq_hbm)

    def tile_at(s):
        return lax.rem(s + me, TILES)

    def w_copy(mat, s):
        slot = lax.rem(mat * TILES + s, SLOTS)
        cols = pl.ds(pl.multiple_of(tile_at(s) * WIDE, WIDE), WIDE)
        return pltpu.make_async_copy(weights[mat].at[:, cols], wbuf.at[slot], wsem.at[slot])

    tok_copy = pltpu.make_async_copy(tok_hbm, tok, tok_sem)
    tok_copy.start()
    for s in range(AHEAD):
        w_copy(0, s).start()

    def prefetch(mat, s):
        later = s + AHEAD

        @pl.when(later < TILES)
        def _():
            w_copy(mat, later).start()

        if mat < 2:
            @pl.when(later >= TILES)
            def _():
                w_copy(mat + 1, later - TILES).start()

    def product(mat, s):
        prefetch(mat, s)
        w_copy(mat, s).wait()
        slot = lax.rem(mat * TILES + s, SLOTS)
        return jnp.dot(x_ref[...], wbuf[slot], preferred_element_type=F32)

    def send_tile(mat, tile, blocks):
        for x in range(4):
            send[mat, tile * 4 + x] = blocks[x]
        for x in range(4):
            dest = pair_device(tile, x)
            src = send.at[mat, tile * 4 + x]
            dst = recv.at[mat, pl.ds(pl.multiple_of(me * ROWS, ROWS), ROWS), :]

            @pl.when(dest != me)
            def _():
                pltpu.make_async_remote_copy(
                    src_ref=src, dst_ref=dst, send_sem=send_sem.at[mat], recv_sem=recv_sem.at[mat],
                    device_id={"seq": dest}, device_id_type=MESH).start()

            @pl.when(dest == me)
            def _():
                pltpu.make_async_copy(src, dst, recv_sem.at[mat]).start()

    lane = lax.broadcasted_iota(jnp.int32, (ROWS, HEAD_DIM), 1)
    pos = lax.broadcasted_iota(jnp.int32, (ROWS, HEAD_DIM), 0) + me * ROWS
    angle = pos.astype(F32) * freq_ref[...]
    sine = jnp.sin(angle)
    tabs[0] = jnp.cos(angle)
    tabs[1] = jnp.where(lane < HEAD_DIM // 2, -sine, sine)

    rows_i = lax.broadcasted_iota(jnp.int32, (PAIR_ROWS, PAIR_ROWS), 0)
    cols_i = lax.broadcasted_iota(jnp.int32, (PAIR_ROWS, PAIR_ROWS), 1)
    apart = (cols_i == 2 * lax.rem(rows_i, ROWS) + rows_i // ROWS).astype(F32).astype(BF16)
    tok_copy.wait()

    def x_step(c, _):
        cols = pl.ds(pl.multiple_of(c * CHUNK, CHUNK), CHUNK)
        y = tok[:, :, cols].reshape(PAIR_ROWS, CHUNK)
        x_ref[:, cols] = jnp.dot(apart, y, preferred_element_type=F32).astype(BF16)
        return 0

    lax.fori_loop(0, D // CHUNK, x_step, 0)
    pl.semaphore_wait(barrier, SEQ_DEV - 1 + TENSOR - 1)

    def v_step(s, _):
        y = product(0, s).astype(BF16)
        send_tile(0, tile_at(s), [y[j * ROWS:(j + 1) * ROWS, hh * 128:(hh + 1) * 128]
                                  for hh in range(2) for j in range(2)])
        return 0

    lax.fori_loop(0, TILES, v_step, 0)

    def kq_step(mat, s, acc):
        y = product(mat, s)
        raw[mat - 1, :, pl.ds(pl.multiple_of(tile_at(s) * WIDE, WIDE), WIDE)] = y
        return acc + (y[:, :128] * y[:, :128] + y[:, 128:] * y[:, 128:])

    eye = rows_i == cols_i

    def ss_copy(mat, d):
        return pltpu.make_async_remote_copy(
            src_ref=ssend.at[mat - 1], dst_ref=srecv.at[mat - 1, d - 1],
            send_sem=ss_send_sem.at[mat - 1, d - 1], recv_sem=ss_sem.at[mat - 1, d - 1],
            device_id={"tensor": lax.rem(t + d, TENSOR)}, device_id_type=MESH)

    def send_sums(mat, acc):
        col = jnp.sum(acc, axis=1, keepdims=True)
        row = jnp.sum(jnp.where(eye, col, 0.0), axis=0, keepdims=True)
        ssend[mat - 1] = jnp.broadcast_to(row, (8, PAIR_ROWS))
        for d in range(1, TENSOR):
            ss_copy(mat, d).start()

    def norm_send(mat, gain_ref):
        total = ssend[mat - 1]
        for d in range(1, TENSOR):
            ss_copy(mat, d).wait_recv()
            total = total + srecv[mat - 1, d - 1]
        col = jnp.sum(jnp.where(eye, total[0:1, :], 0.0), axis=1, keepdims=True)
        scale = lax.rsqrt(col / float(HEADS * HEAD_DIM) + 1e-06)

        def step(s, _):
            tile = tile_at(s)
            cols = pl.ds(pl.multiple_of(tile * WIDE, WIDE), WIDE)
            y = raw[mat - 1, :, cols] * scale * gain_ref[cols][None, :]
            blocks = []
            for hh in range(2):
                for j in range(2):
                    u = y[j * ROWS:(j + 1) * ROWS, hh * 128:(hh + 1) * 128]
                    turned = u * tabs[0] + pltpu.roll(u, HEAD_DIM // 2, 1) * tabs[1]
                    blocks.append(turned.astype(BF16))
            send_tile(mat, tile, blocks)
            return 0

        lax.fori_loop(0, TILES, step, 0)

    zero = jnp.zeros((PAIR_ROWS, 128), F32)
    acc = lax.fori_loop(0, TILES, lambda s, a: kq_step(1, s, a), zero)
    send_sums(1, acc)
    acc = lax.fori_loop(0, 3, lambda s, a: kq_step(2, s, a), zero)
    norm_send(1, gk_ref)
    acc = lax.fori_loop(3, TILES, lambda s, a: kq_step(2, s, a), acc)
    send_sums(2, acc)
    wo_copy = pltpu.make_async_copy(wo_hbm, wobuf, wosem)
    wo_copy.start()
    norm_send(2, gq_ref)

    my_z = me // 4
    my_x = lax.rem(me, 4)
    shifted = lax.rem(my_z + 8 - 2 * my_x + 8, 8)
    my_tile = (5 * shifted + 4) // 8
    attends = (8 * my_tile) // 5 == shifted
    head = my_tile * 2 + my_x // 2
    j_mine = lax.rem(my_x, 2)

    @pl.when(attends)
    def _():
        for mat in range(3):
            pltpu.make_async_copy(recv.at[mat], recv.at[mat], recv_sem.at[mat]).wait()
        scale = float(HEAD_DIM ** -0.5 * np.log2(np.e))
        diag = (lax.broadcasted_iota(jnp.int32, (QB, QB), 0) >= lax.broadcasted_iota(jnp.int32, (QB, QB), 1))
        for b in range(SEQ_DEV * ROWS // QB):
            q = recv[2, b * QB:(b + 1) * QB, :]
            last = lax.dot_general(q, recv[1, b * QB:(b + 1) * QB, :], (((1,), (1,)), ((), ())),
                                   preferred_element_type=F32)
            last = jnp.where(diag, last, -1e30)
            top = jnp.max(last, axis=1, keepdims=True)
            if b > 0:
                past = lax.dot_general(q, recv[1, 0:b * QB, :], (((1,), (1,)), ((), ())),
                                       preferred_element_type=F32)
                top = jnp.maximum(top, jnp.max(past, axis=1, keepdims=True))
                e_past = jnp.exp2((past - top) * scale)
            e_last = jnp.exp2((last - top) * scale)
            total = jnp.sum(e_last, axis=1, keepdims=True)
            o = jnp.dot(e_last.astype(BF16), recv[0, b * QB:(b + 1) * QB, :], preferred_element_type=F32)
            if b > 0:
                total = total + jnp.sum(e_past, axis=1, keepdims=True)
                o = o + jnp.dot(e_past.astype(BF16), recv[0, 0:b * QB, :], preferred_element_type=F32)
            amix[b * QB:(b + 1) * QB, :] = (o / total).astype(BF16)
            for k in range(QB // ROWS):
                dest = b * (QB // ROWS) + k
                src = amix.at[pl.ds(dest * ROWS, ROWS), :]
                dst = mixed.at[pl.ds(pl.multiple_of(j_mine * ROWS, ROWS), ROWS),
                               pl.ds(pl.multiple_of(head * 128, 128), 128)]

                @pl.when(dest != me)
                def _():
                    pltpu.make_async_remote_copy(
                        src_ref=src, dst_ref=dst, send_sem=mix_send_sem, recv_sem=mix_sem,
                        device_id={"seq": jnp.int32(dest)}, device_id_type=MESH).start()

                @pl.when(dest == me)
                def _():
                    pltpu.make_async_copy(src, dst, mix_sem).start()

    wo_copy.wait()
    pltpu.make_async_copy(mixed, mixed, mix_sem).wait()
    swap = (cols_i == lax.rem(rows_i, 2) * ROWS + rows_i // 2).astype(F32).astype(BF16)
    perm[...] = jnp.dot(swap, mixed[...], preferred_element_type=F32).astype(BF16)
    out_rows = PAIR_ROWS // TENSOR

    def o_step(c, _):
        cols = pl.ds(pl.multiple_of(c * CHUNK, CHUNK), CHUNK)
        y = jnp.dot(perm[...], wobuf[:, cols], preferred_element_type=F32)
        part[...] = y
        osend[:, cols] = y.astype(BF16)
        oself[:, cols] = part[pl.ds(pl.multiple_of(t * out_rows, out_rows), out_rows), :]
        for d in range(1, TENSOR):
            peer = lax.rem(t + d, TENSOR)
            pltpu.make_async_remote_copy(
                src_ref=osend.at[pl.ds(pl.multiple_of(peer * out_rows, out_rows), out_rows), cols],
                dst_ref=orecv.at[d - 1, :, cols],
                send_sem=o_send_sem.at[d - 1], recv_sem=o_sem.at[d - 1],
                device_id={"tensor": peer}, device_id_type=MESH).start()
        return 0

    lax.fori_loop(0, D // CHUNK, o_step, 0)
    for d in range(1, TENSOR):
        pltpu.make_async_copy(orecv.at[d - 1], orecv.at[d - 1], o_sem.at[d - 1]).wait()

    def sum_step(c, _):
        cols = pl.ds(pl.multiple_of(c * CHUNK, CHUNK), CHUNK)
        y = oself[:, cols]
        for d in range(1, TENSOR):
            y = y + orecv[d - 1, :, cols].astype(F32)
        out_ref[:, :, cols] = y.astype(BF16).reshape(out_rows // 2, 2, CHUNK)
        return 0

    lax.fori_loop(0, D // CHUNK, sum_step, 0)

    for mat in range(1, 3):
        for d in range(1, TENSOR):
            ss_copy(mat, d).wait_send()
    for d in range(1, TENSOR):
        pltpu.make_async_copy(orecv.at[d - 1], orecv.at[d - 1], o_send_sem.at[d - 1]).wait()

    @pl.when(attends)
    def _():
        for mat in range(3):
            left = send.at[mat, pl.ds(0, 4 * TILES - 1)]
            pltpu.make_async_copy(left, left, send_sem.at[mat]).wait()
        left = amix.at[pl.ds(0, (SEQ_DEV - 1) * ROWS), :]
        pltpu.make_async_copy(left, left, mix_send_sem).wait()

    @pl.when(jnp.logical_not(attends))
    def _():
        for mat in range(3):
            pltpu.make_async_copy(send.at[mat], send.at[mat], send_sem.at[mat]).wait()


def local(tokens, w_query, w_key, w_value, w_out, gain_query, gain_key):
    idx = np.arange(HEAD_DIM, dtype=np.float32) % (HEAD_DIM // 2)
    freqs = np.exp(-np.log(np.float32(500000.0)) * idx * np.float32(2.0) / np.float32(HEAD_DIM))
    freq_row = jnp.asarray(freqs.astype(np.float32)[None, :])
    dma = pltpu.SemaphoreType.DMA
    vmem = pl.BlockSpec(memory_space=pltpu.VMEM)
    hbm = pl.BlockSpec(memory_space=pl.ANY)
    out_rows = PAIR_ROWS // TENSOR
    out = pl.pallas_call(
        kernel,
        out_shape=jax.ShapeDtypeStruct((out_rows // 2, 2, D), BF16),
        in_specs=[hbm] + [vmem] * 3 + [hbm] * 4,
        out_specs=vmem,
        scratch_shapes=[
            pltpu.VMEM((ROWS, 2, D), BF16),
            pltpu.VMEM((PAIR_ROWS, D), BF16),
            pltpu.VMEM((SLOTS, D, WIDE), BF16),
            pltpu.VMEM((LOCAL, D), BF16),
            pltpu.VMEM((2, PAIR_ROWS, LOCAL), F32),
            pltpu.VMEM((3, 4 * TILES, ROWS, 128), BF16),
            pltpu.VMEM((3, SEQ_DEV * ROWS, 128), BF16),
            pltpu.VMEM((SEQ_DEV * ROWS, 128), BF16),
            pltpu.VMEM((PAIR_ROWS, LOCAL), BF16),
            pltpu.VMEM((PAIR_ROWS, LOCAL), BF16),
            pltpu.VMEM((PAIR_ROWS, CHUNK), F32),
            pltpu.VMEM((PAIR_ROWS, D), BF16),
            pltpu.VMEM((TENSOR - 1, out_rows, D), BF16),
            pltpu.VMEM((out_rows, D), F32),
            pltpu.VMEM((2, 8, PAIR_ROWS), F32),
            pltpu.VMEM((2, TENSOR - 1, 8, PAIR_ROWS), F32),
            pltpu.VMEM((2, ROWS, HEAD_DIM), F32),
            dma, dma((SLOTS,)), dma, dma((3,)), dma((3,)), dma, dma,
            dma((2, TENSOR - 1)), dma((2, TENSOR - 1)), dma((TENSOR - 1,)), dma((TENSOR - 1,)),
        ],
        compiler_params=pltpu.CompilerParams(
            collective_id=0, has_side_effects=True, vmem_limit_bytes=60 * 1024 * 1024),
        name="layer",
    )(tokens, gain_query, gain_key, freq_row, w_query, w_key, w_value, w_out)
    return out


def solution(mesh):
    return jax.shard_map(
        local,
        mesh=mesh,
        in_specs=(
            P("seq", "dp", None),
            P(None, "tensor"),
            P(None, "tensor"),
            P(None, "tensor"),
            P("tensor", None),
            P("tensor"),
            P("tensor"),
        ),
        out_specs=P(("seq", "tensor"), "dp", None),
        check_vma=False,
    )
```

```python
import functools

import jax
import jax.numpy as jnp
import numpy as np
from jax import lax
from jax.experimental import pallas as pl
from jax.experimental.pallas import tpu as pltpu
from jax.sharding import PartitionSpec as P

HEADS = 40
HEAD_DIM = 128
D = 5120
SEQ_DEV = 32
TENSOR = 4
ROWS = 64
PAIR_ROWS = 128
LOCAL = 1280
TILES = 5
WIDE = 256
SLOTS = 4
AHEAD = 3
CHUNK = 1280
QB = 256
OWNERS = QB // ROWS
GROUPS = 2
MESH = pl.DeviceIdType.MESH
F32 = jnp.float32
BF16 = jnp.bfloat16


def pair_device(head, j, core):
    x = lax.rem(head + 2 * j, 4)
    z = lax.rem(3 * (head // 4) + lax.rem(head, 4) // 2 + 2 * x + 4 * core, 8)
    return z * 4 + x


def kernel(tok_hbm, gq_hbm, gk_hbm, freq_hbm, wq_hbm, wk_hbm, wv_hbm, wo_hbm, out_ref,
           tok, x_ref, gq_ref, gk_ref, freq_ref, wbuf, wobuf, raw, send, recv, amix, mixed, part, osend, orecv, oself,
           ssend, srecv, tabs, tok_sem, gain_sem, wsem, wosem, send_sem, recv_sem, mix_send_sem, mix_sem,
           ss_send_sem, ss_sem, o_send_sem, o_sem):
    me = lax.axis_index("seq")
    t = lax.axis_index("tensor")
    core = lax.axis_index("dp")
    barrier = pltpu.get_barrier_semaphore()

    weights = (wv_hbm, wk_hbm, wq_hbm)

    def tile_at(s):
        return lax.rem(s + me, TILES)

    def w_copy(mat, s):
        slot = lax.rem(mat * TILES + s, SLOTS)
        cols = pl.ds(pl.multiple_of(tile_at(s) * WIDE, WIDE), WIDE)
        return pltpu.make_async_copy(weights[mat].at[:, cols], wbuf.at[slot], wsem.at[slot])


    tok_copy = pltpu.make_async_copy(tok_hbm, tok, tok_sem)
    tok_copy.start()
    for s in range(AHEAD):
        w_copy(0, s).start()

    small = [pltpu.make_async_copy(a, b, gain_sem.at[k]) for k, (a, b) in
             enumerate(((gq_hbm, gq_ref), (gk_hbm, gk_ref), (freq_hbm, freq_ref)))]
    for copy in small:
        copy.start()

    def greet(d, _):
        pl.semaphore_signal(barrier, inc=1, device_id={"seq": lax.rem(me + d, SEQ_DEV)}, device_id_type=MESH)
        return 0

    lax.fori_loop(1, SEQ_DEV, greet, 0)
    for d in range(1, TENSOR):
        pl.semaphore_signal(barrier, inc=1, device_id={"tensor": lax.rem(t + d, TENSOR)}, device_id_type=MESH)

    def prefetch(mat, s):
        later = s + AHEAD

        @pl.when(later < TILES)
        def _():
            w_copy(mat, later).start()

        if mat < 2:
            @pl.when(later >= TILES)
            def _():
                w_copy(mat + 1, later - TILES).start()

    def product(mat, s):
        prefetch(mat, s)
        w_copy(mat, s).wait()
        slot = lax.rem(mat * TILES + s, SLOTS)
        return jnp.dot(x_ref[...], wbuf[slot], preferred_element_type=F32)

    def start_pair(mat, head, j):
        dest = pair_device(head, j, core)
        src = send.at[mat, head * 2 + j]
        dst = recv.at[mat, me]

        @pl.when(dest != me)
        def _():
            pltpu.make_async_remote_copy(
                src_ref=src, dst_ref=dst, send_sem=send_sem.at[mat], recv_sem=recv_sem.at[mat],
                device_id={"seq": dest}, device_id_type=MESH).start()

        @pl.when(dest == me)
        def _():
            pltpu.make_async_copy(src, dst, recv_sem.at[mat]).start()

    def send_tile(mat, tile, y, sequences):
        y = jnp.dot(apart, y, preferred_element_type=F32).astype(BF16)
        for hh in range(2):
            for j in range(2):
                send[mat, tile * 4 + hh * 2 + j] = y[j * ROWS:(j + 1) * ROWS, hh * 128:(hh + 1) * 128]
        for hh in range(2):
            for j in sequences:
                start_pair(mat, tile * 2 + hh, j)

    rows_i = lax.broadcasted_iota(jnp.int32, (PAIR_ROWS, PAIR_ROWS), 0)
    cols_i = lax.broadcasted_iota(jnp.int32, (PAIR_ROWS, PAIR_ROWS), 1)
    apart = (cols_i == 2 * lax.rem(rows_i, ROWS) + rows_i // ROWS).astype(F32).astype(BF16)
    tok_copy.wait()

    def x_step(c, _):
        cols = pl.ds(pl.multiple_of(c * CHUNK, CHUNK), CHUNK)
        x_ref[:, cols] = tok[:, :, cols].reshape(PAIR_ROWS, CHUNK)
        return 0

    lax.fori_loop(0, D // CHUNK, x_step, 0)

    first = product(0, 0).astype(BF16)
    pl.semaphore_wait(barrier, SEQ_DEV - 1 + TENSOR - 1)
    send_tile(0, tile_at(0), first, (0, 1))

    def v_step(s, _):
        send_tile(0, tile_at(s), product(0, s).astype(BF16), (0, 1))
        return 0

    lax.fori_loop(1, TILES, v_step, 0)

    for copy in small:
        copy.wait()
    lane = lax.broadcasted_iota(jnp.int32, (PAIR_ROWS, HEAD_DIM), 1)
    pos = lax.broadcasted_iota(jnp.int32, (PAIR_ROWS, HEAD_DIM), 0) // 2 + me * ROWS
    angle = pos.astype(F32) * freq_ref[...]
    sine = jnp.sin(angle)
    tabs[0] = jnp.cos(angle)
    tabs[1] = jnp.where(lane < HEAD_DIM // 2, -sine, sine)

    def kq_step(mat, s, acc):
        y = product(mat, s)
        raw[mat - 1, :, pl.ds(pl.multiple_of(tile_at(s) * WIDE, WIDE), WIDE)] = y
        return acc + (y[:, :128] * y[:, :128] + y[:, 128:] * y[:, 128:])

    eye = rows_i == cols_i

    def ss_copy(mat, d):
        return pltpu.make_async_remote_copy(
            src_ref=ssend.at[mat - 1], dst_ref=srecv.at[mat - 1, d - 1],
            send_sem=ss_send_sem.at[mat - 1, d - 1], recv_sem=ss_sem.at[mat - 1, d - 1],
            device_id={"tensor": lax.rem(t + d, TENSOR)}, device_id_type=MESH)

    def send_sums(mat, acc):
        col = jnp.sum(acc, axis=1, keepdims=True)
        row = jnp.sum(jnp.where(eye, col, 0.0), axis=0, keepdims=True)
        ssend[mat - 1] = jnp.broadcast_to(row, (8, PAIR_ROWS))
        for d in range(1, TENSOR):
            ss_copy(mat, d).start()

    def norm_send(mat, gain_ref):
        total = ssend[mat - 1]
        for d in range(1, TENSOR):
            ss_copy(mat, d).wait_recv()
            total = total + srecv[mat - 1, d - 1]
        col = jnp.sum(jnp.where(eye, total[0:1, :], 0.0), axis=1, keepdims=True)
        scale = lax.rsqrt(col / float(HEADS * HEAD_DIM) + 1e-06)

        def step(s, _):
            tile = tile_at(s)
            cols = pl.ds(pl.multiple_of(tile * WIDE, WIDE), WIDE)
            y = raw[mat - 1, :, cols] * scale * gain_ref[cols][None, :]
            turned = []
            for hh in range(2):
                u = y[:, hh * 128:(hh + 1) * 128]
                turned.append((u * tabs[0] + pltpu.roll(u, HEAD_DIM // 2, 1) * tabs[1]).astype(BF16))
            send_tile(mat, tile, jnp.concatenate(turned, axis=1), (0,))
            return 0

        lax.fori_loop(0, TILES, step, 0)

    zero = jnp.zeros((PAIR_ROWS, 128), F32)
    acc = lax.fori_loop(0, TILES, lambda s, a: kq_step(1, s, a), zero)
    send_sums(1, acc)
    acc = lax.fori_loop(0, 3, lambda s, a: kq_step(2, s, a), zero)
    norm_send(1, gk_ref)
    acc = lax.fori_loop(3, TILES, lambda s, a: kq_step(2, s, a), acc)
    send_sums(2, acc)
    wo_copy = pltpu.make_async_copy(wo_hbm, wobuf, wosem)
    wo_copy.start()
    norm_send(2, gq_ref)

    def second(k, _):
        head = lax.rem(k + 2 * me, 2 * TILES)
        start_pair(1, head, 1)
        start_pair(2, head, 1)
        return 0

    lax.fori_loop(0, 2 * TILES, second, 0)

    my_z = me // 4
    my_x = lax.rem(me, 4)
    shifted = lax.rem(my_z + 16 - 2 * my_x - 4 * core, 8)
    group = shifted // 3
    side = lax.rem(shifted, 3)
    attends = jnp.logical_and(side < 2, shifted < 7)
    head = jnp.minimum(4 * group + 2 * side + lax.rem(my_x, 2), 2 * TILES - 1)
    j_mine = lax.rem(my_x // 2 + side, 2)

    @pl.when(attends)
    def _():
        for mat in range(3):
            pltpu.make_async_copy(recv.at[mat], recv.at[mat], recv_sem.at[mat]).wait()
        scale = float(HEAD_DIM ** -0.5 * np.log2(np.e))
        causal = (lax.broadcasted_iota(jnp.int32, (QB, QB), 0) >= lax.broadcasted_iota(jnp.int32, (QB, QB), 1))
        dst = mixed.at[j_mine, :, pl.ds(pl.multiple_of(head * 128, 128), 128)]
        group_size = SEQ_DEV // GROUPS
        for g in range(GROUPS):
            for b in range(g * group_size // OWNERS, (g + 1) * group_size // OWNERS):
                own = slice(b * OWNERS, (b + 1) * OWNERS)
                q = recv[2, own].reshape(QB, HEAD_DIM)
                last = lax.dot_general(q, recv[1, own].reshape(QB, HEAD_DIM), (((1,), (1,)), ((), ())),
                                       preferred_element_type=F32)
                last = jnp.where(causal, last, -1e30)
                top = jnp.max(last, axis=1, keepdims=True)
                if b > 0:
                    past = lax.dot_general(q, recv[1, 0:b * OWNERS].reshape(b * QB, HEAD_DIM),
                                           (((1,), (1,)), ((), ())), preferred_element_type=F32)
                    top = jnp.maximum(top, jnp.max(past, axis=1, keepdims=True))
                    e_past = jnp.exp2((past - top) * scale)
                e_last = jnp.exp2((last - top) * scale)
                total = jnp.sum(e_last, axis=1, keepdims=True)
                o = jnp.dot(e_last.astype(BF16), recv[0, own].reshape(QB, HEAD_DIM), preferred_element_type=F32)
                if b > 0:
                    total = total + jnp.sum(e_past, axis=1, keepdims=True)
                    o = o + jnp.dot(e_past.astype(BF16), recv[0, 0:b * OWNERS].reshape(b * QB, HEAD_DIM),
                                    preferred_element_type=F32)
                amix[own] = (o / total).astype(BF16).reshape(OWNERS, ROWS, HEAD_DIM)

            def give(k, _):
                dest = g * group_size + lax.rem(me + k, group_size)

                @pl.when(dest != me)
                def _():
                    pltpu.make_async_remote_copy(
                        src_ref=amix.at[dest], dst_ref=dst, send_sem=mix_send_sem, recv_sem=mix_sem.at[j_mine],
                        device_id={"seq": dest}, device_id_type=MESH).start()

                @pl.when(dest == me)
                def _():
                    pltpu.make_async_copy(amix.at[dest], dst, mix_sem.at[j_mine]).start()
                return 0

            lax.fori_loop(0, group_size, give, 0)

    wo_copy.wait()
    out_rows = ROWS // TENSOR
    for j in range(2):
        pltpu.make_async_copy(mixed.at[j], mixed.at[j], mix_sem.at[j]).wait()

        def o_step(c, _):
            cols = pl.ds(pl.multiple_of(c * CHUNK, CHUNK), CHUNK)
            y = jnp.dot(mixed[j], wobuf[:, cols], preferred_element_type=F32)
            part[...] = y
            osend[j, :, cols] = y.astype(BF16)

            def rows_of(index):
                return pl.ds(pl.multiple_of(index * out_rows, out_rows), out_rows)

            oself[j, :, cols] = part[rows_of(t), :]
            for d in range(1, TENSOR):
                peer = lax.rem(t + d, TENSOR)
                pltpu.make_async_remote_copy(
                    src_ref=osend.at[j, rows_of(peer), cols], dst_ref=orecv.at[j, d - 1, :, cols],
                    send_sem=o_send_sem.at[j, d - 1], recv_sem=o_sem.at[j, d - 1],
                    device_id={"tensor": peer}, device_id_type=MESH).start()
            return 0

        lax.fori_loop(0, D // CHUNK, o_step, 0)

    for j in range(2):
        for d in range(1, TENSOR):
            pltpu.make_async_copy(orecv.at[j, d - 1], orecv.at[j, d - 1], o_sem.at[j, d - 1]).wait()
    rows_o = lax.broadcasted_iota(jnp.int32, (2 * out_rows, 2 * out_rows), 0)
    cols_o = lax.broadcasted_iota(jnp.int32, (2 * out_rows, 2 * out_rows), 1)
    swap = (cols_o == lax.rem(rows_o, 2) * out_rows + rows_o // 2).astype(F32).astype(BF16)

    def sum_step(c, _):
        cols = pl.ds(pl.multiple_of(c * CHUNK, CHUNK), CHUNK)
        both = []
        for j in range(2):
            y = oself[j, :, cols]
            for d in range(1, TENSOR):
                y = y + orecv[j, d - 1, :, cols].astype(F32)
            both.append(y.astype(BF16))
        y = jnp.dot(swap, jnp.concatenate(both, axis=0), preferred_element_type=F32)
        out_ref[:, :, cols] = y.astype(BF16).reshape(out_rows, 2, CHUNK)
        return 0

    lax.fori_loop(0, D // CHUNK, sum_step, 0)

    for mat in range(1, 3):
        for d in range(1, TENSOR):
            ss_copy(mat, d).wait_send()
    for j in range(2):
        for d in range(1, TENSOR):
            pltpu.make_async_copy(orecv.at[j, d - 1], orecv.at[j, d - 1], o_send_sem.at[j, d - 1]).wait()

    @pl.when(attends)
    def _():
        for mat in range(3):
            left = send.at[mat, pl.ds(0, 4 * TILES - 1)]
            pltpu.make_async_copy(left, left, send_sem.at[mat]).wait()
        left = amix.at[pl.ds(0, SEQ_DEV - 1)]
        pltpu.make_async_copy(left, left, mix_send_sem).wait()

    @pl.when(jnp.logical_not(attends))
    def _():
        for mat in range(3):
            pltpu.make_async_copy(send.at[mat], send.at[mat], send_sem.at[mat]).wait()


def local(tokens, w_query, w_key, w_value, w_out, gain_query, gain_key):
    idx = np.arange(HEAD_DIM, dtype=np.float32) % (HEAD_DIM // 2)
    freqs = np.exp(-np.log(np.float32(500000.0)) * idx * np.float32(2.0) / np.float32(HEAD_DIM))
    freq_row = jnp.asarray(freqs.astype(np.float32)[None, :])
    dma = pltpu.SemaphoreType.DMA
    vmem = pl.BlockSpec(memory_space=pltpu.VMEM)
    hbm = pl.BlockSpec(memory_space=pl.ANY)
    out_rows = ROWS // TENSOR
    out = pl.pallas_call(
        kernel,
        out_shape=jax.ShapeDtypeStruct((ROWS // TENSOR, 2, D), BF16),
        in_specs=[hbm] * 8,
        out_specs=vmem,
        scratch_shapes=[
            pltpu.VMEM((ROWS, 2, D), BF16),
            pltpu.VMEM((PAIR_ROWS, D), BF16),
            pltpu.VMEM((LOCAL,), F32),
            pltpu.VMEM((LOCAL,), F32),
            pltpu.VMEM((1, HEAD_DIM), F32),
            pltpu.VMEM((SLOTS, D, WIDE), BF16),
            pltpu.VMEM((LOCAL, D), BF16),
            pltpu.VMEM((2, PAIR_ROWS, LOCAL), F32),
            pltpu.VMEM((3, 4 * TILES, ROWS, 128), BF16),
            pltpu.VMEM((3, SEQ_DEV, ROWS, 128), BF16),
            pltpu.VMEM((SEQ_DEV, ROWS, 128), BF16),
            pltpu.VMEM((2, ROWS, LOCAL), BF16),
            pltpu.VMEM((ROWS, CHUNK), F32),
            pltpu.VMEM((2, ROWS, D), BF16),
            pltpu.VMEM((2, TENSOR - 1, out_rows, D), BF16),
            pltpu.VMEM((2, out_rows, D), F32),
            pltpu.VMEM((2, 8, PAIR_ROWS), F32),
            pltpu.VMEM((2, TENSOR - 1, 8, PAIR_ROWS), F32),
            pltpu.VMEM((2, PAIR_ROWS, HEAD_DIM), F32),
            dma, dma((3,)), dma((SLOTS,)), dma, dma((3,)), dma((3,)), dma, dma((2,)),
            dma((2, TENSOR - 1)), dma((2, TENSOR - 1)), dma((2, TENSOR - 1)), dma((2, TENSOR - 1)),
        ],
        compiler_params=pltpu.CompilerParams(
            collective_id=0, has_side_effects=True, vmem_limit_bytes=60 * 1024 * 1024),
        name="layer",
    )(tokens, gain_query, gain_key, freq_row, w_query, w_key, w_value, w_out)
    return out


def solution(mesh):
    return jax.shard_map(
        local,
        mesh=mesh,
        in_specs=(
            P("seq", "dp", None),
            P(None, "tensor"),
            P(None, "tensor"),
            P(None, "tensor"),
            P("tensor", None),
            P("tensor"),
            P("tensor"),
        ),
        out_specs=P(("seq", "tensor"), "dp", None),
        check_vma=False,
    )
```

```python
import functools

import jax
import jax.numpy as jnp
import numpy as np
from jax import lax
from jax.experimental import pallas as pl
from jax.experimental.pallas import tpu as pltpu
from jax.sharding import PartitionSpec as P

HEADS = 40
HEAD_DIM = 128
D = 5120
SEQ_DEV = 32
TENSOR = 4
ROWS = 64
PAIR_ROWS = 128
LOCAL = 1280
TILES = 5
WIDE = 256
SLOTS = 4
AHEAD = 3
CHUNK = 1280
QB = 256
OWNERS = QB // ROWS
GROUPS = 4
MESH = pl.DeviceIdType.MESH
F32 = jnp.float32
BF16 = jnp.bfloat16


def pair_device(head, j, core):
    x = lax.rem(head + 2 * j, 4)
    z = lax.rem(3 * (head // 4) + lax.rem(head, 4) // 2 + 2 * x + 4 * core, 8)
    return z * 4 + x


def kernel(tok_hbm, gq_hbm, gk_hbm, freq_hbm, wq_hbm, wk_hbm, wv_hbm, wo_hbm, out_ref,
           tok, x_ref, gq_ref, gk_ref, freq_ref, wbuf, wobuf, raw, send, recv, amix, mixed, part, osend, orecv, oself,
           ssend, srecv, tabs, tok_sem, gain_sem, wsem, wosem, send_sem, recv_sem, mix_send_sem, mix_sem,
           ss_send_sem, ss_sem, o_send_sem, o_sem):
    me = lax.axis_index("seq")
    t = lax.axis_index("tensor")
    core = lax.axis_index("dp")
    barrier = pltpu.get_barrier_semaphore()

    weights = (wv_hbm, wk_hbm, wq_hbm)

    def tile_at(s):
        return lax.rem(s + me, TILES)

    def w_copy(mat, s):
        slot = lax.rem(mat * TILES + s, SLOTS)
        cols = pl.ds(pl.multiple_of(tile_at(s) * WIDE, WIDE), WIDE)
        return pltpu.make_async_copy(weights[mat].at[:, cols], wbuf.at[slot], wsem.at[slot])


    tok_copy = pltpu.make_async_copy(tok_hbm, tok, tok_sem)
    w_copy(0, 0).start()
    tok_copy.start()

    small = [pltpu.make_async_copy(a, b, gain_sem.at[k]) for k, (a, b) in
             enumerate(((gq_hbm, gq_ref), (gk_hbm, gk_ref), (freq_hbm, freq_ref)))]
    for copy in small:
        copy.start()

    def greet(d, _):
        pl.semaphore_signal(barrier, inc=1, device_id={"seq": lax.rem(me + d, SEQ_DEV)}, device_id_type=MESH)
        return 0

    lax.fori_loop(1, SEQ_DEV, greet, 0)
    for d in range(1, TENSOR):
        pl.semaphore_signal(barrier, inc=1, device_id={"tensor": lax.rem(t + d, TENSOR)}, device_id_type=MESH)

    def prefetch(mat, s):
        later = s + AHEAD

        @pl.when(later < TILES)
        def _():
            w_copy(mat, later).start()

        if mat < 2:
            @pl.when(later >= TILES)
            def _():
                w_copy(mat + 1, later - TILES).start()

    def product(mat, s):
        prefetch(mat, s)
        w_copy(mat, s).wait()
        slot = lax.rem(mat * TILES + s, SLOTS)
        return jnp.dot(x_ref[...], wbuf[slot], preferred_element_type=F32)

    def start_pair(mat, head, j):
        dest = pair_device(head, j, core)
        src = send.at[mat, head * 2 + j]
        dst = recv.at[mat, me]

        @pl.when(dest != me)
        def _():
            pltpu.make_async_remote_copy(
                src_ref=src, dst_ref=dst, send_sem=send_sem.at[mat], recv_sem=recv_sem.at[mat],
                device_id={"seq": dest}, device_id_type=MESH).start()

        @pl.when(dest == me)
        def _():
            pltpu.make_async_copy(src, dst, recv_sem.at[mat]).start()

    def keep_tile(mat, tile, y):
        y = jnp.dot(apart, y, preferred_element_type=F32).astype(BF16)
        for hh in range(2):
            for j in range(2):
                send[mat, tile * 4 + hh * 2 + j] = y[j * ROWS:(j + 1) * ROWS, hh * 128:(hh + 1) * 128]

    def send_tile(mat, tile, y):
        keep_tile(mat, tile, y)
        for hh in range(2):
            for j in range(2):
                start_pair(mat, tile * 2 + hh, j)

    def send_sequence(mats, j):
        def step(k, _):
            head = lax.rem(k + 2 * me, 2 * TILES)
            for mat in mats:
                start_pair(mat, head, j)
            return 0

        lax.fori_loop(0, 2 * TILES, step, 0)

    rows_i = lax.broadcasted_iota(jnp.int32, (PAIR_ROWS, PAIR_ROWS), 0)
    cols_i = lax.broadcasted_iota(jnp.int32, (PAIR_ROWS, PAIR_ROWS), 1)
    apart = (cols_i == 2 * lax.rem(rows_i, ROWS) + rows_i // ROWS).astype(F32).astype(BF16)
    tok_copy.wait()
    for s in range(1, AHEAD):
        w_copy(0, s).start()

    def x_step(c, _):
        cols = pl.ds(pl.multiple_of(c * CHUNK, CHUNK), CHUNK)
        x_ref[:, cols] = tok[:, :, cols].reshape(PAIR_ROWS, CHUNK)
        return 0

    lax.fori_loop(0, D // CHUNK, x_step, 0)

    first = product(0, 0).astype(BF16)
    pl.semaphore_wait(barrier, SEQ_DEV - 1 + TENSOR - 1)
    send_tile(0, tile_at(0), first)

    def v_step(s, _):
        send_tile(0, tile_at(s), product(0, s).astype(BF16))
        return 0

    lax.fori_loop(1, TILES, v_step, 0)

    for copy in small:
        copy.wait()
    lane = lax.broadcasted_iota(jnp.int32, (PAIR_ROWS, HEAD_DIM), 1)
    pos = lax.broadcasted_iota(jnp.int32, (PAIR_ROWS, HEAD_DIM), 0) // 2 + me * ROWS
    angle = pos.astype(F32) * freq_ref[...]
    sine = jnp.sin(angle)
    tabs[0] = jnp.cos(angle)
    tabs[1] = jnp.where(lane < HEAD_DIM // 2, -sine, sine)

    def kq_step(mat, s, acc):
        y = product(mat, s)
        raw[mat - 1, :, pl.ds(pl.multiple_of(tile_at(s) * WIDE, WIDE), WIDE)] = y
        return acc + (y[:, :128] * y[:, :128] + y[:, 128:] * y[:, 128:])

    eye = rows_i == cols_i

    def ss_copy(mat, d):
        return pltpu.make_async_remote_copy(
            src_ref=ssend.at[mat - 1], dst_ref=srecv.at[mat - 1, d - 1],
            send_sem=ss_send_sem.at[mat - 1, d - 1], recv_sem=ss_sem.at[mat - 1, d - 1],
            device_id={"tensor": lax.rem(t + d, TENSOR)}, device_id_type=MESH)

    def send_sums(mat, acc):
        col = jnp.sum(acc, axis=1, keepdims=True)
        row = jnp.sum(jnp.where(eye, col, 0.0), axis=0, keepdims=True)
        ssend[mat - 1] = jnp.broadcast_to(row, (8, PAIR_ROWS))
        for d in range(1, TENSOR):
            ss_copy(mat, d).start()

    def norm_send(mat, gain_ref):
        total = ssend[mat - 1]
        for d in range(1, TENSOR):
            ss_copy(mat, d).wait_recv()
            total = total + srecv[mat - 1, d - 1]
        col = jnp.sum(jnp.where(eye, total[0:1, :], 0.0), axis=1, keepdims=True)
        scale = lax.rsqrt(col / float(HEADS * HEAD_DIM) + 1e-06)

        for tile in range(TILES):
            cols = pl.ds(tile * WIDE, WIDE)
            y = raw[mat - 1, :, cols] * scale * gain_ref[cols][None, :]
            turned = []
            for hh in range(2):
                u = y[:, hh * 128:(hh + 1) * 128]
                turned.append((u * tabs[0] + pltpu.roll(u, HEAD_DIM // 2, 1) * tabs[1]).astype(BF16))
            keep_tile(mat, tile, jnp.concatenate(turned, axis=1))
        send_sequence((mat,), 0)

    zero = jnp.zeros((PAIR_ROWS, 128), F32)
    acc = lax.fori_loop(0, TILES, lambda s, a: kq_step(1, s, a), zero)
    send_sums(1, acc)
    acc = lax.fori_loop(0, 3, lambda s, a: kq_step(2, s, a), zero)
    norm_send(1, gk_ref)
    acc = lax.fori_loop(3, TILES, lambda s, a: kq_step(2, s, a), acc)
    send_sums(2, acc)
    wo_copy = pltpu.make_async_copy(wo_hbm, wobuf, wosem)
    wo_copy.start()
    norm_send(2, gq_ref)

    send_sequence((1, 2), 1)

    my_z = me // 4
    my_x = lax.rem(me, 4)
    shifted = lax.rem(my_z + 16 - 2 * my_x - 4 * core, 8)
    group = shifted // 3
    side = lax.rem(shifted, 3)
    attends = jnp.logical_and(side < 2, shifted < 7)
    head = jnp.minimum(4 * group + 2 * side + lax.rem(my_x, 2), 2 * TILES - 1)
    j_mine = lax.rem(my_x // 2 + side, 2)

    @pl.when(attends)
    def _():
        for mat in range(3):
            pltpu.make_async_copy(recv.at[mat], recv.at[mat], recv_sem.at[mat]).wait()
        scale = float(HEAD_DIM ** -0.5 * np.log2(np.e))
        causal = (lax.broadcasted_iota(jnp.int32, (QB, QB), 0) >= lax.broadcasted_iota(jnp.int32, (QB, QB), 1))
        dst = mixed.at[j_mine, :, pl.ds(pl.multiple_of(head * 128, 128), 128)]
        group_size = SEQ_DEV // GROUPS
        for g in range(GROUPS):
            for b in range(g * group_size // OWNERS, (g + 1) * group_size // OWNERS):
                own = slice(b * OWNERS, (b + 1) * OWNERS)
                q = recv[2, own].reshape(QB, HEAD_DIM)
                last = lax.dot_general(q, recv[1, own].reshape(QB, HEAD_DIM), (((1,), (1,)), ((), ())),
                                       preferred_element_type=F32)
                last = jnp.where(causal, last, -1e30)
                top = jnp.max(last, axis=1, keepdims=True)
                if b > 0:
                    past = lax.dot_general(q, recv[1, 0:b * OWNERS].reshape(b * QB, HEAD_DIM),
                                           (((1,), (1,)), ((), ())), preferred_element_type=F32)
                    top = jnp.maximum(top, jnp.max(past, axis=1, keepdims=True))
                    e_past = jnp.exp2((past - top) * scale)
                e_last = jnp.exp2((last - top) * scale)
                total = jnp.sum(e_last, axis=1, keepdims=True)
                o = jnp.dot(e_last.astype(BF16), recv[0, own].reshape(QB, HEAD_DIM), preferred_element_type=F32)
                if b > 0:
                    total = total + jnp.sum(e_past, axis=1, keepdims=True)
                    o = o + jnp.dot(e_past.astype(BF16), recv[0, 0:b * OWNERS].reshape(b * QB, HEAD_DIM),
                                    preferred_element_type=F32)
                amix[own] = (o / total).astype(BF16).reshape(OWNERS, ROWS, HEAD_DIM)

            def give(k, _):
                dest = g * group_size + lax.rem(me + k, group_size)

                @pl.when(dest != me)
                def _():
                    pltpu.make_async_remote_copy(
                        src_ref=amix.at[dest], dst_ref=dst, send_sem=mix_send_sem, recv_sem=mix_sem.at[j_mine],
                        device_id={"seq": dest}, device_id_type=MESH).start()

                @pl.when(dest == me)
                def _():
                    pltpu.make_async_copy(amix.at[dest], dst, mix_sem.at[j_mine]).start()
                return 0

            lax.fori_loop(0, group_size, give, 0)

    wo_copy.wait()
    out_rows = ROWS // TENSOR
    for j in range(2):
        pltpu.make_async_copy(mixed.at[j], mixed.at[j], mix_sem.at[j]).wait()

        def o_step(c, _):
            cols = pl.ds(pl.multiple_of(c * CHUNK, CHUNK), CHUNK)
            y = jnp.dot(mixed[j], wobuf[:, cols], preferred_element_type=F32)
            part[...] = y
            osend[j, :, cols] = y.astype(BF16)

            def rows_of(index):
                return pl.ds(pl.multiple_of(index * out_rows, out_rows), out_rows)

            oself[j, :, cols] = part[rows_of(t), :]
            for d in (2, 1, 3):
                peer = lax.rem(t + d, TENSOR)
                pltpu.make_async_remote_copy(
                    src_ref=osend.at[j, rows_of(peer), cols], dst_ref=orecv.at[j, d - 1, :, cols],
                    send_sem=o_send_sem.at[j, d - 1], recv_sem=o_sem.at[j, d - 1],
                    device_id={"tensor": peer}, device_id_type=MESH).start()
            return 0

        lax.fori_loop(0, D // CHUNK, o_step, 0)

    for j in range(2):
        for d in range(1, TENSOR):
            pltpu.make_async_copy(orecv.at[j, d - 1], orecv.at[j, d - 1], o_sem.at[j, d - 1]).wait()
    rows_o = lax.broadcasted_iota(jnp.int32, (2 * out_rows, 2 * out_rows), 0)
    cols_o = lax.broadcasted_iota(jnp.int32, (2 * out_rows, 2 * out_rows), 1)
    swap = (cols_o == lax.rem(rows_o, 2) * out_rows + rows_o // 2).astype(F32).astype(BF16)

    def sum_step(c, _):
        cols = pl.ds(pl.multiple_of(c * CHUNK, CHUNK), CHUNK)
        both = []
        for j in range(2):
            y = oself[j, :, cols]
            for d in range(1, TENSOR):
                y = y + orecv[j, d - 1, :, cols].astype(F32)
            both.append(y.astype(BF16))
        y = jnp.dot(swap, jnp.concatenate(both, axis=0), preferred_element_type=F32)
        out_ref[:, :, cols] = y.astype(BF16).reshape(out_rows, 2, CHUNK)
        return 0

    lax.fori_loop(0, D // CHUNK, sum_step, 0)

    for mat in range(1, 3):
        for d in range(1, TENSOR):
            ss_copy(mat, d).wait_send()
    for j in range(2):
        for d in range(1, TENSOR):
            pltpu.make_async_copy(orecv.at[j, d - 1], orecv.at[j, d - 1], o_send_sem.at[j, d - 1]).wait()

    @pl.when(attends)
    def _():
        for mat in range(3):
            left = send.at[mat, pl.ds(0, 4 * TILES - 1)]
            pltpu.make_async_copy(left, left, send_sem.at[mat]).wait()
        left = amix.at[pl.ds(0, SEQ_DEV - 1)]
        pltpu.make_async_copy(left, left, mix_send_sem).wait()

    @pl.when(jnp.logical_not(attends))
    def _():
        for mat in range(3):
            pltpu.make_async_copy(send.at[mat], send.at[mat], send_sem.at[mat]).wait()


def write_out(y_ref, out_ref):
    out_ref[...] = y_ref[...]


def local(tokens, w_query, w_key, w_value, w_out, gain_query, gain_key):
    idx = np.arange(HEAD_DIM, dtype=np.float32) % (HEAD_DIM // 2)
    freqs = np.exp(-np.log(np.float32(500000.0)) * idx * np.float32(2.0) / np.float32(HEAD_DIM))
    freq_row = jnp.asarray(freqs.astype(np.float32)[None, :])
    dma = pltpu.SemaphoreType.DMA
    vmem = pl.BlockSpec(memory_space=pltpu.VMEM)
    hbm = pl.BlockSpec(memory_space=pl.ANY)
    out_rows = ROWS // TENSOR
    out = pl.pallas_call(
        kernel,
        out_shape=jax.ShapeDtypeStruct((ROWS // TENSOR, 2, D), BF16),
        in_specs=[hbm] * 8,
        out_specs=vmem,
        scratch_shapes=[
            pltpu.VMEM((ROWS, 2, D), BF16),
            pltpu.VMEM((PAIR_ROWS, D), BF16),
            pltpu.VMEM((LOCAL,), F32),
            pltpu.VMEM((LOCAL,), F32),
            pltpu.VMEM((1, HEAD_DIM), F32),
            pltpu.VMEM((SLOTS, D, WIDE), BF16),
            pltpu.VMEM((LOCAL, D), BF16),
            pltpu.VMEM((2, PAIR_ROWS, LOCAL), F32),
            pltpu.VMEM((3, 4 * TILES, ROWS, 128), BF16),
            pltpu.VMEM((3, SEQ_DEV, ROWS, 128), BF16),
            pltpu.VMEM((SEQ_DEV, ROWS, 128), BF16),
            pltpu.VMEM((2, ROWS, LOCAL), BF16),
            pltpu.VMEM((ROWS, CHUNK), F32),
            pltpu.VMEM((2, ROWS, D), BF16),
            pltpu.VMEM((2, TENSOR - 1, out_rows, D), BF16),
            pltpu.VMEM((2, out_rows, D), F32),
            pltpu.VMEM((2, 8, PAIR_ROWS), F32),
            pltpu.VMEM((2, TENSOR - 1, 8, PAIR_ROWS), F32),
            pltpu.VMEM((2, PAIR_ROWS, HEAD_DIM), F32),
            dma, dma((3,)), dma((SLOTS,)), dma, dma((3,)), dma((3,)), dma, dma((2,)),
            dma((2, TENSOR - 1)), dma((2, TENSOR - 1)), dma((2, TENSOR - 1)), dma((2, TENSOR - 1)),
        ],
        compiler_params=pltpu.CompilerParams(
            collective_id=0, has_side_effects=True, vmem_limit_bytes=60 * 1024 * 1024),
        name="layer",
    )(tokens, gain_query, gain_key, freq_row, w_query, w_key, w_value, w_out)
    return pl.pallas_call(
        write_out,
        out_shape=jax.ShapeDtypeStruct(out.shape, BF16),
        in_specs=[vmem],
        out_specs=vmem,
        name="write_out",
    )(out)


def solution(mesh):
    return jax.shard_map(
        local,
        mesh=mesh,
        in_specs=(
            P("seq", "dp", None),
            P(None, "tensor"),
            P(None, "tensor"),
            P(None, "tensor"),
            P("tensor", None),
            P("tensor"),
            P("tensor"),
        ),
        out_specs=P(("seq", "tensor"), "dp", None),
        check_vma=False,
    )
```

```python
import functools

import jax
import jax.numpy as jnp
import numpy as np
from jax import lax
from jax.experimental import pallas as pl
from jax.experimental.pallas import tpu as pltpu
from jax.sharding import PartitionSpec as P

HEADS = 40
HEAD_DIM = 128
D = 5120
SEQ_DEV = 32
TENSOR = 4
ROWS = 64
PAIR_ROWS = 128
LOCAL = 1280
TILES = 5
WIDE = 256
SLOTS = 4
AHEAD = 3
CHUNK = 1280
QB = 256
GROUPS = 4
PASSES = 2
PASS_ROWS = ROWS // PASSES
PASS_TOKENS = ROWS // TENSOR // PASSES
OWNERS = QB // PASS_ROWS
MESH = pl.DeviceIdType.MESH
F32 = jnp.float32
BF16 = jnp.bfloat16


def pair_device(head, j, core):
    x = lax.rem(head + 2 * j, 4)
    z = lax.rem(3 * (head // 4) + lax.rem(head, 4) // 2 + 2 * x + 4 * core, 8)
    return z * 4 + x


def token_of(row):
    inner = lax.rem(row, PASS_ROWS)
    return inner // PASS_TOKENS * (ROWS // TENSOR) + row // PASS_ROWS * PASS_TOKENS + lax.rem(inner, PASS_TOKENS)


def kernel(tok_hbm, gq_hbm, gk_hbm, freq_hbm, wq_hbm, wk_hbm, wv_hbm, wo_hbm, out_ref,
           tok, x_ref, gq_ref, gk_ref, freq_ref, wbuf, wobuf, raw, send, recv, amix, mixed, part, osend, orecv, oself,
           ssend, srecv, tabs, tok_sem, gain_sem, wsem, wosem, send_sem, recv_sem, mix_send_sem, mix_sem,
           ss_send_sem, ss_sem, o_send_sem, o_sem):
    me = lax.axis_index("seq")
    t = lax.axis_index("tensor")
    core = lax.axis_index("dp")
    barrier = pltpu.get_barrier_semaphore()

    weights = (wv_hbm, wk_hbm, wq_hbm)

    def tile_at(s):
        return lax.rem(s + me, TILES)

    def w_copy(mat, s):
        slot = lax.rem(mat * TILES + s, SLOTS)
        cols = pl.ds(pl.multiple_of(tile_at(s) * WIDE, WIDE), WIDE)
        return pltpu.make_async_copy(weights[mat].at[:, cols], wbuf.at[slot], wsem.at[slot])


    tok_copy = pltpu.make_async_copy(tok_hbm, tok, tok_sem)
    w_copy(0, 0).start()
    tok_copy.start()

    small = [pltpu.make_async_copy(a, b, gain_sem.at[k]) for k, (a, b) in
             enumerate(((gq_hbm, gq_ref), (gk_hbm, gk_ref), (freq_hbm, freq_ref)))]
    for copy in small:
        copy.start()

    def greet(d, _):
        pl.semaphore_signal(barrier, inc=1, device_id={"seq": lax.rem(me + d, SEQ_DEV)}, device_id_type=MESH)
        return 0

    lax.fori_loop(1, SEQ_DEV, greet, 0)
    for d in range(1, TENSOR):
        pl.semaphore_signal(barrier, inc=1, device_id={"tensor": lax.rem(t + d, TENSOR)}, device_id_type=MESH)

    def prefetch(mat, s):
        later = s + AHEAD

        @pl.when(later < TILES)
        def _():
            w_copy(mat, later).start()

        if mat < 2:
            @pl.when(later >= TILES)
            def _():
                w_copy(mat + 1, later - TILES).start()

    def product(mat, s):
        prefetch(mat, s)
        w_copy(mat, s).wait()
        slot = lax.rem(mat * TILES + s, SLOTS)
        return jnp.dot(x_ref[...], wbuf[slot], preferred_element_type=F32)

    def start_pair(mat, head, j):
        dest = pair_device(head, j, core)
        src = send.at[mat, head * 2 + j]
        dst = recv.at[mat, me]

        @pl.when(dest != me)
        def _():
            pltpu.make_async_remote_copy(
                src_ref=src, dst_ref=dst, send_sem=send_sem.at[mat], recv_sem=recv_sem.at[mat],
                device_id={"seq": dest}, device_id_type=MESH).start()

        @pl.when(dest == me)
        def _():
            pltpu.make_async_copy(src, dst, recv_sem.at[mat]).start()

    def keep_tile(mat, tile, y):
        y = jnp.dot(apart, y, preferred_element_type=F32).astype(BF16)
        for hh in range(2):
            for j in range(2):
                send[mat, tile * 4 + hh * 2 + j] = y[j * ROWS:(j + 1) * ROWS, hh * 128:(hh + 1) * 128]

    def send_tile(mat, tile, y):
        keep_tile(mat, tile, y)
        for hh in range(2):
            for j in range(2):
                start_pair(mat, tile * 2 + hh, j)

    def send_sequence(mats, j):
        def step(k, _):
            head = lax.rem(k + 2 * me, 2 * TILES)
            for mat in mats:
                start_pair(mat, head, j)
            return 0

        lax.fori_loop(0, 2 * TILES, step, 0)

    rows_i = lax.broadcasted_iota(jnp.int32, (PAIR_ROWS, PAIR_ROWS), 0)
    cols_i = lax.broadcasted_iota(jnp.int32, (PAIR_ROWS, PAIR_ROWS), 1)
    apart = (cols_i == 2 * token_of(lax.rem(rows_i, ROWS)) + rows_i // ROWS).astype(F32).astype(BF16)
    tok_copy.wait()
    for s in range(1, AHEAD):
        w_copy(0, s).start()

    def x_step(c, _):
        cols = pl.ds(pl.multiple_of(c * CHUNK, CHUNK), CHUNK)
        x_ref[:, cols] = tok[:, :, cols].reshape(PAIR_ROWS, CHUNK)
        return 0

    lax.fori_loop(0, D // CHUNK, x_step, 0)

    first = product(0, 0).astype(BF16)
    pl.semaphore_wait(barrier, SEQ_DEV - 1 + TENSOR - 1)
    send_tile(0, tile_at(0), first)

    def v_step(s, _):
        send_tile(0, tile_at(s), product(0, s).astype(BF16))
        return 0

    lax.fori_loop(1, TILES, v_step, 0)

    for copy in small:
        copy.wait()
    lane = lax.broadcasted_iota(jnp.int32, (PAIR_ROWS, HEAD_DIM), 1)
    pos = lax.broadcasted_iota(jnp.int32, (PAIR_ROWS, HEAD_DIM), 0) // 2 + me * ROWS
    angle = pos.astype(F32) * freq_ref[...]
    sine = jnp.sin(angle)
    tabs[0] = jnp.cos(angle)
    tabs[1] = jnp.where(lane < HEAD_DIM // 2, -sine, sine)

    def kq_step(mat, s, acc):
        y = product(mat, s)
        raw[mat - 1, :, pl.ds(pl.multiple_of(tile_at(s) * WIDE, WIDE), WIDE)] = y
        return acc + (y[:, :128] * y[:, :128] + y[:, 128:] * y[:, 128:])

    eye = rows_i == cols_i

    def ss_copy(mat, d):
        return pltpu.make_async_remote_copy(
            src_ref=ssend.at[mat - 1], dst_ref=srecv.at[mat - 1, d - 1],
            send_sem=ss_send_sem.at[mat - 1, d - 1], recv_sem=ss_sem.at[mat - 1, d - 1],
            device_id={"tensor": lax.rem(t + d, TENSOR)}, device_id_type=MESH)

    def send_sums(mat, acc):
        col = jnp.sum(acc, axis=1, keepdims=True)
        row = jnp.sum(jnp.where(eye, col, 0.0), axis=0, keepdims=True)
        ssend[mat - 1] = jnp.broadcast_to(row, (8, PAIR_ROWS))
        for d in range(1, TENSOR):
            ss_copy(mat, d).start()

    def norm_send(mat, gain_ref):
        total = ssend[mat - 1]
        for d in range(1, TENSOR):
            ss_copy(mat, d).wait_recv()
            total = total + srecv[mat - 1, d - 1]
        col = jnp.sum(jnp.where(eye, total[0:1, :], 0.0), axis=1, keepdims=True)
        scale = lax.rsqrt(col / float(HEADS * HEAD_DIM) + 1e-06)

        for tile in range(TILES):
            cols = pl.ds(tile * WIDE, WIDE)
            y = raw[mat - 1, :, cols] * scale * gain_ref[cols][None, :]
            turned = []
            for hh in range(2):
                u = y[:, hh * 128:(hh + 1) * 128]
                turned.append((u * tabs[0] + pltpu.roll(u, HEAD_DIM // 2, 1) * tabs[1]).astype(BF16))
            keep_tile(mat, tile, jnp.concatenate(turned, axis=1))
        send_sequence((mat,), 0)

    zero = jnp.zeros((PAIR_ROWS, 128), F32)
    acc = lax.fori_loop(0, TILES, lambda s, a: kq_step(1, s, a), zero)
    send_sums(1, acc)
    acc = lax.fori_loop(0, 3, lambda s, a: kq_step(2, s, a), zero)
    norm_send(1, gk_ref)
    acc = lax.fori_loop(3, TILES, lambda s, a: kq_step(2, s, a), acc)
    send_sums(2, acc)
    wo_copy = pltpu.make_async_copy(wo_hbm, wobuf, wosem)
    wo_copy.start()
    norm_send(2, gq_ref)

    send_sequence((1, 2), 1)

    my_z = me // 4
    my_x = lax.rem(me, 4)
    shifted = lax.rem(my_z + 16 - 2 * my_x - 4 * core, 8)
    group = shifted // 3
    side = lax.rem(shifted, 3)
    attends = jnp.logical_and(side < 2, shifted < 7)
    head = jnp.minimum(4 * group + 2 * side + lax.rem(my_x, 2), 2 * TILES - 1)
    j_mine = lax.rem(my_x // 2 + side, 2)

    @pl.when(attends)
    def _():
        for mat in range(3):
            pltpu.make_async_copy(recv.at[mat], recv.at[mat], recv_sem.at[mat]).wait()
        scale = float(HEAD_DIM ** -0.5 * np.log2(np.e))
        span = OWNERS * ROWS
        q_row = lax.broadcasted_iota(jnp.int32, (QB, 1), 0)
        k_row = lax.broadcasted_iota(jnp.int32, (1, span), 1)
        k_pos = k_row // ROWS * ROWS + token_of(lax.rem(k_row, ROWS))
        cols = pl.ds(pl.multiple_of(head * 128, 128), 128)
        group_size = SEQ_DEV // GROUPS
        for g in range(GROUPS):
            for p in range(PASSES):
                q_pos = q_row // PASS_ROWS * ROWS + token_of(p * PASS_ROWS + lax.rem(q_row, PASS_ROWS))
                for b in range(g * group_size // OWNERS, (g + 1) * group_size // OWNERS):
                    own = slice(b * OWNERS, (b + 1) * OWNERS)
                    q = recv[2, own, p * PASS_ROWS:(p + 1) * PASS_ROWS, :].reshape(QB, HEAD_DIM)
                    last = lax.dot_general(q, recv[1, own].reshape(span, HEAD_DIM), (((1,), (1,)), ((), ())),
                                           preferred_element_type=F32)
                    last = jnp.where(q_pos >= k_pos, last, -1e30)
                    top = jnp.max(last, axis=1, keepdims=True)
                    if b > 0:
                        past = lax.dot_general(q, recv[1, 0:b * OWNERS].reshape(b * span, HEAD_DIM),
                                               (((1,), (1,)), ((), ())), preferred_element_type=F32)
                        top = jnp.maximum(top, jnp.max(past, axis=1, keepdims=True))
                        e_past = jnp.exp2((past - top) * scale)
                    e_last = jnp.exp2((last - top) * scale)
                    total = jnp.sum(e_last, axis=1, keepdims=True)
                    o = jnp.dot(e_last.astype(BF16), recv[0, own].reshape(span, HEAD_DIM),
                                preferred_element_type=F32)
                    if b > 0:
                        total = total + jnp.sum(e_past, axis=1, keepdims=True)
                        o = o + jnp.dot(e_past.astype(BF16), recv[0, 0:b * OWNERS].reshape(b * span, HEAD_DIM),
                                        preferred_element_type=F32)
                    amix[p, own] = (o / total).astype(BF16).reshape(OWNERS, PASS_ROWS, HEAD_DIM)
                dst = mixed.at[j_mine, p * PASS_ROWS:(p + 1) * PASS_ROWS, cols]

                def give(k, _):
                    dest = g * group_size + lax.rem(me + k, group_size)

                    @pl.when(dest != me)
                    def _():
                        pltpu.make_async_remote_copy(
                            src_ref=amix.at[p, dest], dst_ref=dst, send_sem=mix_send_sem.at[p],
                            recv_sem=mix_sem.at[j_mine, p], device_id={"seq": dest}, device_id_type=MESH).start()

                    @pl.when(dest == me)
                    def _():
                        pltpu.make_async_copy(amix.at[p, dest], dst, mix_sem.at[j_mine, p]).start()
                    return 0

                lax.fori_loop(0, group_size, give, 0)

    wo_copy.wait()
    out_rows = ROWS // TENSOR
    for j, passes in ((0, (0, 1)), (1, (0,)), (1, (1,))):
        for p in passes:
            part_rows = mixed.at[j, p * PASS_ROWS:(p + 1) * PASS_ROWS]
            pltpu.make_async_copy(part_rows, part_rows, mix_sem.at[j, p]).wait()
        low, count = passes[0] * PASS_ROWS, len(passes) * PASS_ROWS

        def o_step(c, _):
            cols = pl.ds(pl.multiple_of(c * CHUNK, CHUNK), CHUNK)
            y = jnp.dot(mixed[j, low:low + count], wobuf[:, cols], preferred_element_type=F32)
            part[0:count] = y
            osend[j, low:low + count, cols] = y.astype(BF16)
            for p in passes:
                def rows_of(index, base):
                    return pl.ds(pl.multiple_of(p * PASS_ROWS - base + index * PASS_TOKENS, PASS_TOKENS), PASS_TOKENS)

                place = slice(p * PASS_TOKENS, (p + 1) * PASS_TOKENS)
                oself[j, place, cols] = part[rows_of(t, low), :]
                for d in (2, 1, 3):
                    peer = lax.rem(t + d, TENSOR)
                    pltpu.make_async_remote_copy(
                        src_ref=osend.at[j, rows_of(peer, 0), cols], dst_ref=orecv.at[j, d - 1, place, cols],
                        send_sem=o_send_sem.at[j, d - 1], recv_sem=o_sem.at[j, d - 1],
                        device_id={"tensor": peer}, device_id_type=MESH).start()
            return 0

        lax.fori_loop(0, D // CHUNK, o_step, 0)

    for j in range(2):
        for d in range(1, TENSOR):
            pltpu.make_async_copy(orecv.at[j, d - 1], orecv.at[j, d - 1], o_sem.at[j, d - 1]).wait()
    rows_o = lax.broadcasted_iota(jnp.int32, (2 * out_rows, 2 * out_rows), 0)
    cols_o = lax.broadcasted_iota(jnp.int32, (2 * out_rows, 2 * out_rows), 1)
    swap = (cols_o == lax.rem(rows_o, 2) * out_rows + rows_o // 2).astype(F32).astype(BF16)

    def sum_step(c, _):
        cols = pl.ds(pl.multiple_of(c * CHUNK, CHUNK), CHUNK)
        both = []
        for j in range(2):
            y = oself[j, :, cols]
            for d in range(1, TENSOR):
                y = y + orecv[j, d - 1, :, cols].astype(F32)
            both.append(y.astype(BF16))
        y = jnp.dot(swap, jnp.concatenate(both, axis=0), preferred_element_type=F32)
        out_ref[:, :, cols] = y.astype(BF16).reshape(out_rows, 2, CHUNK)
        return 0

    lax.fori_loop(0, D // CHUNK, sum_step, 0)

    for mat in range(1, 3):
        for d in range(1, TENSOR):
            ss_copy(mat, d).wait_send()
    for j in range(2):
        for d in range(1, TENSOR):
            pltpu.make_async_copy(orecv.at[j, d - 1], orecv.at[j, d - 1], o_send_sem.at[j, d - 1]).wait()

    @pl.when(attends)
    def _():
        for mat in range(3):
            left = send.at[mat, pl.ds(0, 4 * TILES - 1)]
            pltpu.make_async_copy(left, left, send_sem.at[mat]).wait()
        for p in range(PASSES):
            left = amix.at[p, pl.ds(0, SEQ_DEV - 1)]
            pltpu.make_async_copy(left, left, mix_send_sem.at[p]).wait()

    @pl.when(jnp.logical_not(attends))
    def _():
        for mat in range(3):
            pltpu.make_async_copy(send.at[mat], send.at[mat], send_sem.at[mat]).wait()


def write_out(y_ref, out_ref):
    out_ref[...] = y_ref[...]


def local(tokens, w_query, w_key, w_value, w_out, gain_query, gain_key):
    idx = np.arange(HEAD_DIM, dtype=np.float32) % (HEAD_DIM // 2)
    freqs = np.exp(-np.log(np.float32(500000.0)) * idx * np.float32(2.0) / np.float32(HEAD_DIM))
    freq_row = jnp.asarray(freqs.astype(np.float32)[None, :])
    dma = pltpu.SemaphoreType.DMA
    vmem = pl.BlockSpec(memory_space=pltpu.VMEM)
    hbm = pl.BlockSpec(memory_space=pl.ANY)
    out_rows = ROWS // TENSOR
    out = pl.pallas_call(
        kernel,
        out_shape=jax.ShapeDtypeStruct((ROWS // TENSOR, 2, D), BF16),
        in_specs=[hbm] * 8,
        out_specs=vmem,
        scratch_shapes=[
            pltpu.VMEM((ROWS, 2, D), BF16),
            pltpu.VMEM((PAIR_ROWS, D), BF16),
            pltpu.VMEM((LOCAL,), F32),
            pltpu.VMEM((LOCAL,), F32),
            pltpu.VMEM((1, HEAD_DIM), F32),
            pltpu.VMEM((SLOTS, D, WIDE), BF16),
            pltpu.VMEM((LOCAL, D), BF16),
            pltpu.VMEM((2, PAIR_ROWS, LOCAL), F32),
            pltpu.VMEM((3, 4 * TILES, ROWS, 128), BF16),
            pltpu.VMEM((3, SEQ_DEV, ROWS, 128), BF16),
            pltpu.VMEM((PASSES, SEQ_DEV, PASS_ROWS, 128), BF16),
            pltpu.VMEM((2, ROWS, LOCAL), BF16),
            pltpu.VMEM((ROWS, CHUNK), F32),
            pltpu.VMEM((2, ROWS, D), BF16),
            pltpu.VMEM((2, TENSOR - 1, out_rows, D), BF16),
            pltpu.VMEM((2, out_rows, D), F32),
            pltpu.VMEM((2, 8, PAIR_ROWS), F32),
            pltpu.VMEM((2, TENSOR - 1, 8, PAIR_ROWS), F32),
            pltpu.VMEM((2, PAIR_ROWS, HEAD_DIM), F32),
            dma, dma((3,)), dma((SLOTS,)), dma, dma((3,)), dma((3,)), dma((PASSES,)), dma((2, PASSES)),
            dma((2, TENSOR - 1)), dma((2, TENSOR - 1)), dma((2, TENSOR - 1)), dma((2, TENSOR - 1)),
        ],
        compiler_params=pltpu.CompilerParams(
            collective_id=0, has_side_effects=True, vmem_limit_bytes=60 * 1024 * 1024),
        name="layer",
    )(tokens, gain_query, gain_key, freq_row, w_query, w_key, w_value, w_out)
    return pl.pallas_call(
        write_out,
        out_shape=jax.ShapeDtypeStruct(out.shape, BF16),
        in_specs=[vmem],
        out_specs=vmem,
        name="write_out",
    )(out)


def solution(mesh):
    return jax.shard_map(
        local,
        mesh=mesh,
        in_specs=(
            P("seq", "dp", None),
            P(None, "tensor"),
            P(None, "tensor"),
            P(None, "tensor"),
            P("tensor", None),
            P("tensor"),
            P("tensor"),
        ),
        out_specs=P(("seq", "tensor"), "dp", None),
        check_vma=False,
    )
```
